32 devices in a mesh: aa: 4 (over x, core), ba: 4 (over z), col: 2 (over y).
Axes of the slice: x: 2, y: 2, z: 4, core: 2. Of those that a mesh axis runs over, the one named last changes fastest.
Arguments:
- tokens: bfloat16 [64, 32, 64, 1024], P('aa', 'ba', 'col'), may hold values from -6 to 6
- norm_gain: float32 [1024], replicated, may hold values from 0.1 to 1.9
- in_weight: bfloat16 [1024, 3072], replicated, may hold values from -0.1875 to 0.1875
- skip_gain: float32 [1024], replicated, may hold values from 0.5 to 1.5
- spectrum_filter: bfloat16 [2, 64, 32, 64, 1024], P(None, ('ba', 'col'), None, None, 'aa'), may hold values from -4 to 4
- out_weight: bfloat16 [1024, 1024], replicated, may hold values from -0.1875 to 0.1875
Outputs:
- layer_out: bfloat16 [64, 32, 64, 1024], P('aa', 'ba', 'col')
The draws below stay inside these ranges and needn't reach their ends.
All inputs are finite; a program needn't handle non-finite values.
Results may differ from the reference program's by a relative error of at most 0.014.
Values may be sent and summed in bfloat16 or wider, within the bound.
No kernel may reach another device: no remote copies, remote signals or barrier semaphores. Data moves between devices by JAX's collectives and lax.ppermute only.
A program may use at most 256 MiB of HBM per device.

```python
import math
import jax
import jax.numpy as jnp
from jax import lax

LA = 64
LB = 32
LC = 64
D = 1024


def steps_of(own_key, extent, split, smallest, largest):
    def one(dim, shards_of):
        heights = jax.random.uniform(jax.random.fold_in(jax.random.fold_in(own_key, 6), dim), (shards_of,), jnp.float32, smallest / len(split), largest / len(split))
        return jnp.repeat(jnp.exp(heights), extent[dim] // shards_of).reshape((-1,) + (1,) * (len(extent) - dim - 1))

    gain = one(*split[0])
    for cut in split[1:]:
        gain = gain * one(*cut)
    return gain


def centred(stream_key, shape, width, limit, pieces=(), kind=jnp.bfloat16):
    values = width * jax.random.normal(stream_key, shape, jnp.float32)
    if pieces:
        values = values * steps_of(stream_key, shape, pieces, -0.22, 0.18)
    return jnp.clip(values, -limit, limit).astype(kind)


def setup_inputs(seed: int = 0) -> dict:
    splits = jax.random.split(jax.random.key(seed), 7)
    return {
        "tokens": centred(splits[0], (LA, LB, LC, D), 1.0, 6.0, ((0, 4), (1, 4), (2, 2))),
        "norm_gain": jnp.clip(1.0 + 0.18 * jax.random.normal(splits[1], (D,), jnp.float32), 0.1, 1.9),
        "in_weight": centred(splits[2], (D, 3 * D), D ** -0.5, 0.1875),
        "skip_gain": jnp.clip(jax.random.uniform(splits[3], (D,), jnp.float32, 0.5, 1.5), 0.5, 1.5),
        "spectrum_filter": centred(splits[4], (2, LA, LB, LC, D), 0.7, 4.0, ((1, 8), (4, 4))),
        "out_weight": centred(splits[5], (D, D), D ** -0.5, 0.1875),
    }


EPSILON = 1e-06

def dft_tables(length):
    counter = jnp.arange(length, dtype=jnp.int32)
    product = counter[:, None] * counter[None, :] % length
    angle = 2.0 * math.pi / length * product.astype(jnp.float32)
    factor = 1.0 / math.sqrt(length)
    cos_table = (jnp.cos(angle) * factor).astype(jnp.bfloat16).astype(jnp.float32)
    sin_table = (jnp.sin(angle) * factor).astype(jnp.bfloat16).astype(jnp.float32)
    return (cos_table, sin_table)

def phase_pair(integer_phase, modulus):
    angle = 2.0 * math.pi / modulus * (integer_phase % modulus).astype(jnp.float32)
    return (jnp.cos(angle), jnp.sin(angle))

def rounded(value):
    return lax.optimization_barrier(value.astype(jnp.bfloat16)).astype(jnp.float32)

def reference(tokens, norm_gain, in_weight, skip_gain, spectrum_filter, out_weight):
    points = LA * LB * LC
    rows = tokens.reshape(LA, LB * LC, D)

    def project(block):
        flat = block.astype(jnp.float32)
        meansq = lax.optimization_barrier(jnp.mean(flat * flat, axis=-1, keepdims=True))
        normed = (flat * lax.rsqrt(meansq + EPSILON) * norm_gain).astype(jnp.bfloat16)
        projected = jnp.dot(normed, in_weight, preferred_element_type=jnp.float32)
        mixed_rows = (projected[:, :D] * projected[:, 2 * D:]).astype(jnp.bfloat16)
        gate_rows = projected[:, D:2 * D].astype(jnp.bfloat16)
        return (mixed_rows, gate_rows)
    mixed, gate = lax.map(project, rows)
    cos_a, sin_a = dft_tables(LA)
    cos_b, sin_b = dft_tables(LB)
    cos_c, sin_c = dft_tables(LC)
    freq_a = jnp.arange(LA, dtype=jnp.int32)
    index_j = jnp.arange(LB, dtype=jnp.int32)
    index_k = jnp.arange(LC, dtype=jnp.int32)
    cos_phi, sin_phi = phase_pair((LC * index_j[None, :, None] + index_k[None, None, :]) * freq_a[:, None, None], points)
    cos_phi = cos_phi[..., None]
    sin_phi = sin_phi[..., None]
    cos_psi, sin_psi = phase_pair(index_j[:, None] * index_k[None, :], LB * LC)
    cos_psi = cos_psi[None, :, :, None]
    sin_psi = sin_psi[None, :, :, None]
    group = 128 if D % 128 == 0 else D
    ngroups = D // group
    mixed_groups = mixed.reshape(LA, LB, LC, ngroups, group).transpose(3, 0, 1, 2, 4)
    filter_groups = spectrum_filter.reshape(2, LA, LB, LC, ngroups, group).transpose(4, 0, 1, 2, 3, 5)

    def spectral(operands):
        block, filt = operands
        source = block.astype(jnp.float32)
        real_part = jnp.einsum('fi,ijkc->fjkc', cos_a, source)
        imag_part = -jnp.einsum('fi,ijkc->fjkc', sin_a, source)
        first_real = rounded(real_part * cos_phi + imag_part * sin_phi)
        first_imag = rounded(imag_part * cos_phi - real_part * sin_phi)
        real_part = jnp.einsum('gj,fjkc->fgkc', cos_b, first_real) + jnp.einsum('gj,fjkc->fgkc', sin_b, first_imag)
        imag_part = jnp.einsum('gj,fjkc->fgkc', cos_b, first_imag) - jnp.einsum('gj,fjkc->fgkc', sin_b, first_real)
        second_real = rounded(real_part * cos_psi + imag_part * sin_psi)
        second_imag = rounded(imag_part * cos_psi - real_part * sin_psi)
        spec_real = jnp.einsum('hk,fgkc->fghc', cos_c, second_real) + jnp.einsum('hk,fgkc->fghc', sin_c, second_imag)
        spec_imag = jnp.einsum('hk,fgkc->fghc', cos_c, second_imag) - jnp.einsum('hk,fgkc->fghc', sin_c, second_real)
        filt_real = filt[0].astype(jnp.float32)
        filt_imag = filt[1].astype(jnp.float32)
        filtered_real = rounded(filt_real * spec_real - filt_imag * spec_imag)
        filtered_imag = rounded(filt_real * spec_imag + filt_imag * spec_real)
        real_part = jnp.einsum('hk,fghc->fgkc', cos_c, filtered_real) - jnp.einsum('hk,fghc->fgkc', sin_c, filtered_imag)
        imag_part = jnp.einsum('hk,fghc->fgkc', cos_c, filtered_imag) + jnp.einsum('hk,fghc->fgkc', sin_c, filtered_real)
        third_real = rounded(real_part * cos_psi - imag_part * sin_psi)
        third_imag = rounded(imag_part * cos_psi + real_part * sin_psi)
        real_part = jnp.einsum('gj,fgkc->fjkc', cos_b, third_real) - jnp.einsum('gj,fgkc->fjkc', sin_b, third_imag)
        imag_part = jnp.einsum('gj,fgkc->fjkc', cos_b, third_imag) + jnp.einsum('gj,fgkc->fjkc', sin_b, third_real)
        back_real = rounded(real_part * cos_phi - imag_part * sin_phi)
        back_imag = rounded(imag_part * cos_phi + real_part * sin_phi)
        result = jnp.einsum('fi,fjkc->ijkc', cos_a, back_real) - jnp.einsum('fi,fjkc->ijkc', sin_a, back_imag)
        return result.astype(jnp.bfloat16)
    conv_groups = lax.map(spectral, (mixed_groups, filter_groups))
    conv = conv_groups.transpose(1, 2, 3, 0, 4).reshape(LA, LB * LC, D)

    def finish(operands):
        conv_rows, gate_rows, mixed_rows = operands
        gated = (gate_rows.astype(jnp.float32) * (conv_rows.astype(jnp.float32) + skip_gain * mixed_rows.astype(jnp.float32))).astype(jnp.bfloat16)
        return jnp.dot(gated, out_weight, preferred_element_type=jnp.float32).astype(jnp.bfloat16)
    layer_out = lax.map(finish, (conv, gate, mixed))
    return layer_out.reshape(LA, LB, LC, D)
```

```python
import math

import jax
import jax.numpy as jnp
from jax import lax
from jax.experimental import pallas as pl
from jax.experimental.pallas import tpu as pltpu
from jax.sharding import PartitionSpec as P

LA = 64
LB = 32
LC = 64
D = 1024


EPSILON = 1e-06


def dft_tables(length):
    counter = jnp.arange(length, dtype=jnp.int32)
    product = counter[:, None] * counter[None, :] % length
    angle = 2.0 * math.pi / length * product.astype(jnp.float32)
    factor = 1.0 / math.sqrt(length)
    return (
        (jnp.cos(angle) * factor).astype(jnp.bfloat16),
        (jnp.sin(angle) * factor).astype(jnp.bfloat16),
    )


def phase_pair(integer_phase, modulus):
    angle = 2.0 * math.pi / modulus * (integer_phase % modulus).astype(jnp.float32)
    return (jnp.cos(angle), jnp.sin(angle))


SUB = 16
CHUNKS = 2
TILE = 512
F32 = jnp.float32
BF16 = jnp.bfloat16


def params():
    return pltpu.CompilerParams(vmem_limit_bytes=56 * 1024 * 1024)


def dot(left, right):
    return jnp.dot(left, right, preferred_element_type=F32)


def with_identity(table):
    rows, cols = table.shape[-2:]
    tall = jnp.repeat(table, SUB, axis=-2)
    spread = (jnp.arange(cols)[:, None] == jnp.arange(cols * SUB)[None, :] // SUB).astype(BF16)
    wide = jnp.matmul(tall, spread, preferred_element_type=F32)
    same = jnp.arange(rows * SUB)[:, None] % SUB == jnp.arange(cols * SUB)[None, :] % SUB
    return jnp.where(same, wide, 0.0).astype(BF16)


def project(tokens, norm_gain, in_weight, parts, width):
    count, dim = tokens.shape
    sub = width // CHUNKS

    def kernel(tokens_ref, gain_ref, weight_ref, *outs):
        gate_ref = outs[-1]
        flat = tokens_ref[...].astype(F32)
        meansq = jnp.mean(flat * flat, axis=-1, keepdims=True)
        normed = (flat * lax.rsqrt(meansq + EPSILON) * gain_ref[...]).astype(BF16)
        for part in range(parts):
            at = part * width
            first = dot(normed, weight_ref[:, at : at + width])
            value = dot(normed, weight_ref[:, 2 * dim + at : 2 * dim + at + width])
            mixed = (first * value).astype(BF16)
            for chunk in range(CHUNKS):
                outs[chunk][part] = mixed[:, chunk * sub : (chunk + 1) * sub]
            gate_ref[:, at : at + width] = dot(normed, weight_ref[:, dim + at : dim + at + width]).astype(BF16)

    mixed_spec = pl.BlockSpec((parts, TILE, sub), lambda t: (0, t, 0))
    return pl.pallas_call(
        kernel,
        grid=(count // TILE,),
        in_specs=[
            pl.BlockSpec((TILE, dim), lambda t: (t, 0)),
            pl.BlockSpec((1, dim), lambda t: (0, 0)),
            pl.BlockSpec((dim, 3 * dim), lambda t: (0, 0)),
        ],
        out_specs=[mixed_spec] * CHUNKS + [pl.BlockSpec((TILE, dim), lambda t: (t, 0))],
        out_shape=[jax.ShapeDtypeStruct((parts, count, sub), BF16)] * CHUNKS
        + [jax.ShapeDtypeStruct((count, dim), BF16)],
        compiler_params=params(),
        cost_estimate=pl.CostEstimate(
            flops=6 * count * dim * dim, bytes_accessed=6 * count * dim + 6 * dim * dim, transcendentals=count
        ),
        name="project",
    )(tokens, norm_gain.reshape(1, dim), in_weight)


def finish(convs, mixes, gate, skip_gain, out_weight):
    count, dim = gate.shape
    parts, _, sub = convs[0].shape

    def kernel(*refs):
        conv_refs = refs[:CHUNKS]
        mix_refs = refs[CHUNKS : 2 * CHUNKS]
        gate_ref, skip_ref, weight_ref, out_ref = refs[2 * CHUNKS :]
        pieces = []
        for part in range(parts):
            for chunk in range(CHUNKS):
                at = (part * CHUNKS + chunk) * sub
                conv = conv_refs[chunk][part].astype(F32)
                mixed = mix_refs[chunk][part].astype(F32)
                gate_piece = gate_ref[:, at : at + sub].astype(F32)
                pieces.append((gate_piece * (conv + skip_ref[:, at : at + sub] * mixed)).astype(BF16))
        out_ref[...] = dot(jnp.concatenate(pieces, axis=1), weight_ref[...]).astype(BF16)

    chunk_spec = pl.BlockSpec((parts, TILE, sub), lambda t: (0, t, 0))
    return pl.pallas_call(
        kernel,
        grid=(count // TILE,),
        in_specs=[chunk_spec] * (2 * CHUNKS)
        + [
            pl.BlockSpec((TILE, dim), lambda t: (t, 0)),
            pl.BlockSpec((1, dim), lambda t: (0, 0)),
            pl.BlockSpec((dim, dim), lambda t: (0, 0)),
        ],
        out_specs=pl.BlockSpec((TILE, dim), lambda t: (t, 0)),
        out_shape=jax.ShapeDtypeStruct((count, dim), BF16),
        compiler_params=params(),
        cost_estimate=pl.CostEstimate(
            flops=2 * count * dim * dim, bytes_accessed=8 * count * dim + 2 * dim * dim, transcendentals=0
        ),
        name="finish",
    )(*convs, *mixes, gate, skip_gain.reshape(1, dim), out_weight)


def outer_digit(table, values, name):
    lead, rows_j, rows_k, sub = values.shape
    out_lead = table.shape[0] // SUB

    def kernel(table_ref, values_ref, out_ref):
        block = values_ref[...].reshape(lead * SUB, sub)
        out_ref[...] = dot(table_ref[...], block).astype(BF16).reshape(out_lead, 1, SUB, sub)

    return pl.pallas_call(
        kernel,
        grid=(rows_j, rows_k // SUB),
        in_specs=[
            pl.BlockSpec(table.shape, lambda j, k: (0, 0)),
            pl.BlockSpec((lead, 1, SUB, sub), lambda j, k: (0, j, k, 0)),
        ],
        out_specs=pl.BlockSpec((out_lead, 1, SUB, sub), lambda j, k: (0, j, k, 0)),
        out_shape=jax.ShapeDtypeStruct((out_lead, rows_j, rows_k, sub), BF16),
        compiler_params=params(),
        cost_estimate=pl.CostEstimate(
            flops=2 * table.shape[0] * table.shape[1] * rows_j * (rows_k // SUB) * sub,
            bytes_accessed=2 * (lead + out_lead) * rows_j * rows_k * sub,
            transcendentals=0,
        ),
        name=name,
    )(table, values)


def inner_digits(values, filters, chunk, two, two_back, three, three_back):
    count_ba, count_col, _, freq_local, rows_j, rows_k, sub = values.shape
    groups = rows_k // SUB

    def kernel(values_ref, filter_ref, two_ref, two_back_ref, three_ref, three_back_ref, out_ref, mid_ref):
        for col in range(count_col):
            for group in range(groups):
                inside = slice(group * SUB, (group + 1) * SUB)
                at = col * rows_k + group * SUB
                block = values_ref[:, col, :, 0, :, inside, :].reshape(count_ba * 2 * rows_j * SUB, sub)
                mid_ref[:, :, at : at + SUB, :] = dot(two_ref[0], block).astype(BF16).reshape(2, LB, SUB, sub)
        for index in range(LB):
            block = mid_ref[:, index].reshape(2 * LC, sub)
            spectrum = dot(three_ref[0, index], block)
            spec_real = spectrum[:LC]
            spec_imag = spectrum[LC:]
            filt_real = filter_ref[0, 0, index].astype(F32)
            filt_imag = filter_ref[1, 0, index].astype(F32)
            filtered = jnp.concatenate(
                [filt_real * spec_real - filt_imag * spec_imag, filt_real * spec_imag + filt_imag * spec_real]
            ).astype(BF16)
            mid_ref[:, index] = dot(three_back_ref[0, index], filtered).astype(BF16).reshape(2, LC, sub)
        for col in range(count_col):
            for group in range(groups):
                inside = slice(group * SUB, (group + 1) * SUB)
                at = col * rows_k + group * SUB
                block = mid_ref[:, :, at : at + SUB, :].reshape(2 * LB * SUB, sub)
                back = dot(two_back_ref[0], block).astype(BF16)
                out_ref[:, col, :, 0, :, inside, :] = back.reshape(count_ba, 2, rows_j, SUB, sub)

    shape = (count_ba, count_col, 2, 1, rows_j, rows_k, sub)
    size = 2 * LB * SUB
    moved_spec = pl.BlockSpec(shape, lambda f: (0, 0, 0, f, 0, 0, 0))
    points = freq_local * LB * LC * sub
    return pl.pallas_call(
        kernel,
        grid=(freq_local,),
        in_specs=[
            moved_spec,
            pl.BlockSpec((2, 1, LB, LC, sub), lambda f: (0, f, 0, 0, chunk)),
            pl.BlockSpec((1, size, size), lambda f: (f, 0, 0)),
            pl.BlockSpec((1, size, size), lambda f: (f, 0, 0)),
            pl.BlockSpec((1, LB, 2 * LC, 2 * LC), lambda f: (f, 0, 0, 0)),
            pl.BlockSpec((1, LB, 2 * LC, 2 * LC), lambda f: (f, 0, 0, 0)),
        ],
        out_specs=moved_spec,
        out_shape=jax.ShapeDtypeStruct(values.shape, BF16),
        scratch_shapes=[pltpu.VMEM((2, LB, LC, sub), BF16)],
        compiler_params=params(),
        cost_estimate=pl.CostEstimate(
            flops=4 * points * (2 * size + 4 * LC), bytes_accessed=12 * points, transcendentals=0
        ),
        name="inner_digits",
    )(values, filters, two, two_back, three, three_back)


def local(tokens, norm_gain, in_weight, skip_gain, spectrum_filter, out_weight):
    count_aa = lax.axis_size("aa")
    count_ba = lax.axis_size("ba")
    count_col = lax.axis_size("col")
    rows_i = LA // count_aa
    rows_j = LB // count_ba
    rows_k = LC // count_col
    blocks = count_ba * count_col
    freq_local = LA // blocks
    channels = D // count_aa
    sub = channels // CHUNKS
    points = LA * LB * LC
    count = rows_i * rows_j * rows_k

    *mixes, gate = project(tokens.reshape(count, D), norm_gain, in_weight, count_aa, channels)

    cos_a, sin_a = lax.optimization_barrier(dft_tables(LA))
    pair_a = jnp.stack([cos_a.reshape(blocks, freq_local, LA), -sin_a.reshape(blocks, freq_local, LA)], axis=1)
    pair_a = pair_a.reshape(2 * LA, LA)
    one = with_identity(pair_a)
    one_back = with_identity(pair_a.T)

    slot = lax.axis_index("ba") * count_col + lax.axis_index("col")
    freq = slot * freq_local + jnp.arange(freq_local, dtype=jnp.int32)
    index_j = jnp.arange(LB, dtype=jnp.int32)
    index_k = jnp.arange(LC, dtype=jnp.int32)
    cos_b, sin_b = (table.astype(F32)[None] for table in dft_tables(LB))
    cos_j, sin_j = phase_pair(freq[:, None] * index_j[None, :], LA * LB)
    cos_j, sin_j = cos_j[:, None, :], sin_j[:, None, :]
    real_b = cos_b * cos_j - sin_b * sin_j
    imag_b = -(cos_b * sin_j + sin_b * cos_j)
    block_b = jnp.stack([jnp.stack([real_b, -imag_b], axis=2), jnp.stack([imag_b, real_b], axis=2)], axis=1)
    block_b = block_b.reshape(freq_local, 2, LB, 2, count_ba, rows_j).transpose(0, 1, 2, 4, 3, 5)
    block_b = block_b.reshape(freq_local, 2 * LB, 2 * LB).astype(BF16)
    two = with_identity(block_b)
    two_back = with_identity(block_b.swapaxes(1, 2))

    cos_c, sin_c = (table.astype(F32)[None, None] for table in dft_tables(LC))
    whole = freq[:, None, None] + LA * index_j[None, :, None]
    cos_k, sin_k = phase_pair(whole * index_k[None, None, :], points)

    def third(cos_k, sin_k):
        real_c = cos_c * cos_k - sin_c * sin_k
        imag_c = -(cos_c * sin_k + sin_c * cos_k)
        return real_c, imag_c

    def joined(a, b, c, d):
        return jnp.concatenate([jnp.concatenate([a, b], axis=-1), jnp.concatenate([c, d], axis=-1)], axis=-2).astype(BF16)

    real_c, imag_c = third(cos_k[:, :, None, :], sin_k[:, :, None, :])
    three = joined(real_c, -imag_c, imag_c, real_c)
    real_t, imag_t = third(cos_k[:, :, :, None], sin_k[:, :, :, None])
    three_back = joined(real_t, imag_t, -imag_t, real_t)

    rows = [lax.all_to_all(mixed, "aa", split_axis=0, concat_axis=0, tiled=True) for mixed in mixes]
    moved = []
    for chunk in range(CHUNKS):
        first = outer_digit(one, rows[chunk].reshape(LA, rows_j, rows_k, sub), "first_digit")
        first = first.reshape(blocks, 2, freq_local, rows_j, rows_k, sub)
        moved.append(lax.all_to_all(first, ("ba", "col"), split_axis=0, concat_axis=0, tiled=True))
    returned = []
    for chunk in range(CHUNKS):
        values = moved[chunk].reshape(count_ba, count_col, 2, freq_local, rows_j, rows_k, sub)
        back = inner_digits(values, spectrum_filter, chunk, two, two_back, three, three_back)
        back = back.reshape(blocks, 2, freq_local, rows_j, rows_k, sub)
        returned.append(lax.all_to_all(back, ("ba", "col"), split_axis=0, concat_axis=0, tiled=True))
    convs = []
    for chunk in range(CHUNKS):
        conv = outer_digit(one_back, returned[chunk].reshape(2 * LA, rows_j, rows_k, sub), "last_digit")
        conv = conv.reshape(count_aa, count, sub)
        convs.append(lax.all_to_all(conv, "aa", split_axis=0, concat_axis=0, tiled=True))
    layer_out = finish(convs, mixes, gate, skip_gain, out_weight)
    return layer_out.reshape(rows_i, rows_j, rows_k, D)


def solution(mesh):
    in_specs = (
        P("aa", "ba", "col", None),
        P(),
        P(),
        P(),
        P(None, ("ba", "col"), None, None, "aa"),
        P(),
    )
    out_specs = P("aa", "ba", "col", None)
    return jax.shard_map(local, mesh=mesh, in_specs=in_specs, out_specs=out_specs, check_vma=False)
```
